32 devices in a mesh: ang: 16 (over z, y, x), slab: 2 (over core).
Axes of the slice: x: 2, y: 2, z: 4, core: 2. Of those that a mesh axis runs over, the one named last changes fastest.
Arguments:
- updates: float32 [64, 2, 256, 512], P('ang', None, 'slab'), may hold values from -6 to 6
- interp_tiles: bfloat16 [64, 32, 256, 128], P('ang'), may hold values from -0.1875 to 0.1875
- band_start: int32 [64, 32], P('ang'), may hold values from 0 to 2
- angle_id: int32 [64], P('ang'), may hold values from 0 to 63, each once
- angle_weight: float32 [64], replicated, may hold values from 0.05 to 0.5
- volume: float32 [4096, 2, 256], P('ang', None, 'slab'), may hold values from -6 to 6
Outputs:
- volume_next: float32 [4096, 2, 256], P('ang', None, 'slab')
- projection: float32 [64, 2, 256, 512], P('ang', None, 'slab')
The draws below stay inside these ranges and needn't reach their ends.
Inputs may be any that keep to these rules, and one draw needn't show every extreme that they name: Tile j of angle slot a reads detector columns 128 * band_start[a, j] up to 256 further. `angle_id`: each measured angle stands in exactly one slot.
All inputs are finite; a program needn't handle non-finite values.
Results may differ from the reference program's by a relative error of at most 0.0062.
Values may be sent and summed in bfloat16 or wider, within the bound.
A program may use at most 128 MiB of HBM per device.

```python
import math
import jax
import jax.numpy as jnp
from jax import lax

S = 512
BLOCK = 128
BAND = 256
XW = 8
ANGLES = 64
Z = 256
CELLS = 4096
TILES = 32


def with_ends(entries, own_key, low, largest):
    index_at = [jax.random.randint(jax.random.fold_in(own_key, axis), (), 0, length) for axis, length in enumerate(entries.shape)]
    longest = entries.shape.index(max(entries.shape))
    beside = index_at[:longest] + [(index_at[longest] + 1) % entries.shape[longest]] + index_at[longest + 1:]
    return entries.at[tuple(index_at)].set(low).at[tuple(beside)].set(largest)


def strengthened(values, stream_key, source, target, parts, factor):
    owner, partner = [(jnp.arange(values.shape[dim]) // (values.shape[dim] // parts)).reshape([-1 if axis == dim else 1 for axis in range(values.ndim)]) for dim in (source, target)]
    chosen = jax.random.permutation(stream_key, parts)[partner]
    strong = (owner == chosen) | (owner == (partner + parts // 2) % parts)
    return jnp.where(strong, factor * values, values)


def steps_of(rng, shape, pieces, smallest, largest):
    factor_of, own = 1.0, jax.random.fold_in(rng, 6)
    for position, blocks in pieces:
        steps = jnp.exp(jax.random.uniform(jax.random.fold_in(own, position), (blocks,), jnp.float32, smallest / len(pieces), largest / len(pieces)))
        factor_of = factor_of * jnp.repeat(steps, shape[position] // blocks).reshape([-1 if axis == position else 1 for axis in range(len(shape))])
    return factor_of


def gaussian(key, extent, spread, most, pieces=(), kind=jnp.bfloat16):
    drawn = spread * jax.random.normal(key, extent, jnp.float32)
    if pieces:
        drawn = drawn * steps_of(key, extent, pieces, -0.22, 0.18)
    return jnp.clip(drawn, -most, most).astype(kind)


def noise_with(rng, extent, scale, bound, pieces, heavy, held_as=jnp.bfloat16):
    values = scale * jax.random.normal(rng, extent, jnp.float32)
    if pieces:
        values = values * steps_of(rng, extent, pieces, -0.22, 0.18)
    return jnp.clip(strengthened(values, jax.random.fold_in(rng, 3), *heavy), -bound, bound).astype(held_as)


def setup_inputs(seed: int = 0) -> dict:
    streams_of = jax.random.split(jax.random.key(seed), 7)
    updates = gaussian(streams_of[0], (ANGLES, 2, Z, S), 1.0, 6.0, ((0, 16), (2, 2)), jnp.float32)
    interp_tiles = noise_with(streams_of[1], (ANGLES, TILES, BAND, BLOCK), (BAND * XW) ** -0.5, 0.1875, ((0, 16),), (0, 1, 16, 2.0))
    band_start = with_ends(jax.random.randint(streams_of[2], (ANGLES, TILES), 0, S // BLOCK - 1), jax.random.fold_in(streams_of[2], 1), 0, (S // BLOCK - 1) - 1).astype(jnp.int32)
    angle_id = jax.random.permutation(streams_of[3], ANGLES).astype(jnp.int32)
    angle_weight = jnp.clip(jnp.exp(jax.random.uniform(streams_of[4], (ANGLES,), jnp.float32, math.log(0.05), math.log(0.5))), 0.05, 0.5)
    volume = gaussian(streams_of[5], (CELLS, 2, Z), 1.0, 6.0, ((0, 16), (2, 2)), jnp.float32)
    return dict(updates=updates, interp_tiles=interp_tiles, band_start=band_start, angle_id=angle_id, angle_weight=angle_weight, volume=volume)


SMOOTHING = 0.25


def clamp_absorption(field):
    channel = jnp.arange(2, dtype=jnp.int32)[None, :, None]
    return jnp.where(channel == 1, jnp.maximum(field, 0.0), field)


def band_windows(row_block, starts):
    def take_window(first_block):
        return lax.dynamic_slice_in_dim(row_block, first_block * BLOCK, BAND, axis=1)
    return jax.vmap(take_window)(starts)


def place_bands(images, starts):
    positions = jnp.arange(S // BLOCK - 1, dtype=jnp.int32)
    onehot = (starts[:, None] == positions[None, :]).astype(jnp.float32)
    grouped = jnp.einsum('jk,jrq->krq', onehot, images, precision=lax.Precision.HIGHEST)
    result = jnp.zeros((images.shape[1], S), jnp.float32)
    for offset_index in range(S // BLOCK - 1):
        result = result + jnp.pad(grouped[offset_index], ((0, 0), (BLOCK * offset_index, S - BLOCK * offset_index - BAND)))
    return result


def reference(updates, interp_tiles, band_start, angle_id, angle_weight, volume):
    row_count = 2 * Z
    matches = angle_id[:, None] == jnp.arange(ANGLES, dtype=jnp.int32)[None, :]
    chosen = jnp.sum(jnp.where(matches, angle_weight[None, :], 0.0), axis=1)
    scaled = (chosen[:, None, None, None] * updates).astype(jnp.bfloat16).reshape(ANGLES, row_count, S)

    def back_step(summed, packed):
        row_block, tile_set, starts = packed
        windows = band_windows(row_block, starts).astype(jnp.float32)
        term = jnp.einsum('jrq,jqp->jpr', windows, tile_set.astype(jnp.float32))
        return summed + term, 0

    initial = jnp.zeros((TILES, BLOCK, row_count), jnp.float32)
    summed = lax.scan(back_step, initial, (scaled, interp_tiles, band_start))[0]
    partial_sum = summed.reshape(CELLS, 2, Z)
    padded = jnp.pad(volume, ((0, 0), (0, 0), (1, 1)))
    smooth = volume - SMOOTHING * (2.0 * volume - padded[:, :, :-2] - padded[:, :, 2:])
    volume_next = clamp_absorption(smooth + partial_sum)
    lowered = lax.optimization_barrier(volume_next.astype(jnp.bfloat16))
    lowered = lowered.astype(jnp.float32).reshape(TILES, BLOCK, row_count)

    def forward_one(packed):
        tile_set, starts = packed
        images = jnp.einsum('jpr,jqp->jrq', lowered, tile_set.astype(jnp.float32))
        return place_bands(images, starts)

    projection = lax.map(forward_one, (interp_tiles, band_start))
    return volume_next, projection.reshape(ANGLES, 2, Z, S)
```

```python
import functools

import jax
import jax.numpy as jnp
from jax import lax
from jax.experimental import pallas as pl
from jax.experimental.pallas import tpu as pltpu
from jax.sharding import PartitionSpec as P

SMOOTHING = 0.25
MESH = pl.DeviceIdType.MESH


def kernel(
    groups,
    slabs,
    turns,
    starts_ref,
    ids_ref,
    weights_ref,
    updates_ref,
    tiles_hbm,
    volume_ref,
    next_ref,
    projection_ref,
    tiles_ref,
    wide_ref,
    scaled_ref,
    sent_ref,
    landed_ref,
    gathered_ref,
    halo_ref,
    tile_sems,
    send_sem,
    land_sems,
    spread_sem,
    gather_sems,
    halo_sems,
):
    local_angles, row_count, detector = updates_ref.shape
    tile_count, band_width, block_size = tiles_ref.shape[1:]
    share = sent_ref.shape[2]
    unit = wide_ref.shape[2]
    unit_count = wide_ref.shape[0]
    per_unit = unit // share
    unit_tiles = unit // block_size
    depth = row_count // 2
    column_blocks = detector // block_size
    halves = band_width // block_size
    me = lax.axis_index("ang")
    slab = lax.axis_index("slab")
    my_unit = me // per_unit

    def unit_at(step):
        return lax.rem(my_unit + step, unit_count)

    def tile_copy(where):
        block = pl.ds(where * unit_tiles, unit_tiles)
        return pltpu.make_async_copy(
            tiles_hbm.at[:, block], tiles_ref.at[:, block], tile_sems.at[where]
        )

    @pl.loop(1, unit_count + 1)
    def _(step):
        tile_copy(unit_at(step)).start()

    barrier = pltpu.get_barrier_semaphore()

    @pl.loop(1, groups)
    def _(step):
        peer = lax.rem(me + step, groups)
        pl.semaphore_signal(barrier, inc=1, device_id=(peer, slab), device_id_type=MESH)

    for turn in turns:
        beside = lax.rem(slab + turn, slabs)
        pl.semaphore_signal(barrier, inc=1, device_id=(me, beside), device_id_type=MESH)

    for angle in range(local_angles):
        chosen = weights_ref[ids_ref[angle]]
        scaled_ref[:, angle * detector : (angle + 1) * detector] = (
            chosen * updates_ref[angle]
        ).astype(jnp.bfloat16)

    pl.semaphore_wait(barrier, groups - 1 + len(turns))

    halo_copies = []
    for slot, turn in enumerate(turns):
        halo_copies.append(
            pltpu.make_async_remote_copy(
                src_ref=volume_ref,
                dst_ref=halo_ref.at[slot],
                send_sem=halo_sems.at[0, slot],
                recv_sem=halo_sems.at[1, slot],
                device_id=(me, lax.rem(slab + turn, slabs)),
                device_id_type=MESH,
            )
        )
        halo_copies[-1].start()

    def term_copy(owner):
        return pltpu.make_async_remote_copy(
            src_ref=sent_ref.at[owner],
            dst_ref=landed_ref.at[me],
            send_sem=send_sem.at[owner],
            recv_sem=land_sems.at[me],
            device_id=(owner, slab),
            device_id_type=MESH,
        )

    def back(where):
        tile_copy(where).wait()
        for angle in range(local_angles):
            for part in range(unit_tiles):
                index = where * unit_tiles + part
                first = starts_ref[angle, index]
                for column in range(column_blocks):
                    block = jnp.zeros((block_size, block_size), jnp.bfloat16)
                    for half in range(halves):
                        held = tiles_ref[
                            angle, index, half * block_size : (half + 1) * block_size, :
                        ]
                        block = jnp.where(first + half == column, held, block)
                    top = angle * detector + column * block_size
                    wide_ref[
                        where,
                        top : top + block_size,
                        part * block_size : (part + 1) * block_size,
                    ] = block
        term = jnp.dot(
            scaled_ref[...], wide_ref[where], preferred_element_type=jnp.float32
        ).astype(jnp.bfloat16)
        for part in range(per_unit):
            sent_ref[where * per_unit + part] = term[:, part * share : (part + 1) * share]

    @pl.loop(1, unit_count)
    def _(step):
        where = unit_at(step)
        back(where)
        for part in range(per_unit):
            term_copy(where * per_unit + part).start()

    back(my_unit)
    if per_unit > 1:
        for part in range(per_unit):
            owner = my_unit * per_unit + part

            @pl.when(owner != me)
            def _():
                term_copy(owner).start()

    landed_ref[me] = sent_ref[me]

    def land_wait(step):
        source = lax.rem(me + groups - step, groups)
        pltpu.make_async_remote_copy(
            src_ref=sent_ref.at[source],
            dst_ref=landed_ref.at[source],
            send_sem=send_sem.at[source],
            recv_sem=land_sems.at[source],
            device_id=(source, slab),
            device_id_type=MESH,
        ).wait_recv()

    pl.loop(1, groups)(land_wait)
    for halo_copy in halo_copies:
        halo_copy.wait()

    lane = lax.broadcasted_iota(jnp.int32, (share, depth), 1)
    for channel in range(2):
        rows = slice(channel * depth, (channel + 1) * depth)
        total = lax.fori_loop(
            1,
            groups,
            lambda i, acc: acc + landed_ref[i, rows, :].astype(jnp.float32),
            landed_ref[0, rows, :].astype(jnp.float32),
        )
        if share % 128:
            room = 128 - share % 128
            total = jnp.concatenate([total, jnp.zeros((depth, room), jnp.float32)], axis=1)
        total = total.T[:share]
        cells = volume_ref[:, channel, :]
        before = pltpu.roll(cells, 1, 1)
        after = pltpu.roll(cells, depth - 1, 1)
        edge_before = jnp.zeros_like(cells)
        edge_after = jnp.zeros_like(cells)
        if slabs > 1:
            lower = halo_ref[0, :, channel, :]
            upper = halo_ref[len(turns) - 1, :, channel, :]
            edge_before = jnp.where(slab > 0, pltpu.roll(lower, 1, 1), edge_before)
            edge_after = jnp.where(
                slab < slabs - 1, pltpu.roll(upper, depth - 1, 1), edge_after
            )
        before = jnp.where(lane == 0, edge_before, before)
        after = jnp.where(lane == depth - 1, edge_after, after)
        smooth = cells - SMOOTHING * (2.0 * cells - before - after)
        result = smooth + total
        if channel == 1:
            result = jnp.maximum(result, 0.0)
        next_ref[:, channel, :] = result
        if share % 128:
            room = 128 - share % 128
            result = jnp.concatenate([result, jnp.zeros((room, depth), jnp.float32)], axis=0)
        gathered_ref[me, rows, :] = result.T[:, :share].astype(jnp.bfloat16)

    def spread_copy(peer, slot):
        return pltpu.make_async_remote_copy(
            src_ref=gathered_ref.at[slot],
            dst_ref=gathered_ref.at[slot],
            send_sem=spread_sem.at[peer],
            recv_sem=gather_sems.at[slot],
            device_id=(peer, slab),
            device_id_type=MESH,
        )

    @pl.loop(1, groups)
    def _(step):
        spread_copy(lax.rem(me + step, groups), me).start()

    def forward(where, fresh):
        for angle in range(local_angles):
            image = None
            for part in range(per_unit):
                piece = lax.dot_general(
                    gathered_ref[where * per_unit + part],
                    wide_ref[
                        where,
                        angle * detector : (angle + 1) * detector,
                        part * share : (part + 1) * share,
                    ],
                    (((1,), (1,)), ((), ())),
                    preferred_element_type=jnp.float32,
                )
                image = piece if image is None else image + piece
            if fresh:
                projection_ref[angle] = image
            else:
                projection_ref[angle] += image

    def gather_wait(source):
        spread_copy(source, source).wait_recv()

    if per_unit > 1:
        for part in range(per_unit):
            owner = my_unit * per_unit + part

            @pl.when(owner != me)
            def _():
                gather_wait(owner)

    forward(my_unit, True)

    @pl.loop(1, unit_count)
    def _(step):
        where = lax.rem(my_unit + unit_count - step, unit_count)
        for part in range(per_unit):
            gather_wait(where * per_unit + part)
        forward(where, False)

    @pl.loop(1, groups)
    def _(step):
        peer = lax.rem(me + step, groups)
        term_copy(peer).wait_send()
        spread_copy(peer, me).wait_send()


def shards(groups, slabs, updates, interp_tiles, band_start, angle_id, angle_weight, volume):
    local_angles, channels, depth, detector = updates.shape
    tile_count, band_width, block_size = interp_tiles.shape[1:]
    share = volume.shape[0]
    row_count = channels * depth
    unit = max(share, block_size)
    unit_count = tile_count * block_size // unit
    turns = {1: (), 2: (1,)}.get(slabs, (1, slabs - 1))
    slots = max(1, len(turns))
    half = jnp.bfloat16
    vmem = pl.BlockSpec(memory_space=pltpu.VMEM)
    smem = pl.BlockSpec(memory_space=pltpu.SMEM)
    dma = pltpu.SemaphoreType.DMA
    volume_next, projection = pl.pallas_call(
        functools.partial(kernel, groups, slabs, turns),
        name="project",
        out_shape=(
            jax.ShapeDtypeStruct(volume.shape, jnp.float32),
            jax.ShapeDtypeStruct((local_angles, row_count, detector), jnp.float32),
        ),
        in_specs=[smem, smem, smem, vmem, pl.BlockSpec(memory_space=pl.ANY), vmem],
        out_specs=(vmem, vmem),
        scratch_shapes=[
            pltpu.VMEM(interp_tiles.shape, half),
            pltpu.VMEM((unit_count, local_angles * detector, unit), half),
            pltpu.VMEM((row_count, local_angles * detector), half),
            pltpu.VMEM((groups, row_count, share), half),
            pltpu.VMEM((groups, row_count, share), half),
            pltpu.VMEM((groups, row_count, share), half),
            pltpu.VMEM((slots,) + volume.shape, jnp.float32),
            dma((unit_count,)),
            dma((groups,)),
            dma((groups,)),
            dma((groups,)),
            dma((groups,)),
            dma((2, slots)),
        ],
        compiler_params=pltpu.CompilerParams(
            collective_id=0, has_side_effects=True, vmem_limit_bytes=60 * 1024 * 1024
        ),
    )(
        band_start,
        angle_id,
        angle_weight,
        updates.reshape(local_angles, row_count, detector),
        interp_tiles,
        volume,
    )
    return volume_next, projection.reshape(updates.shape)


def solution(mesh):
    placed = (
        P("ang", None, "slab", None),
        P("ang", None, None, None),
        P("ang", None),
        P("ang"),
        P(),
        P("ang", None, "slab"),
    )
    return jax.shard_map(
        functools.partial(shards, mesh.shape["ang"], mesh.shape["slab"]),
        mesh=mesh,
        in_specs=placed,
        out_specs=(P("ang", None, "slab"), P("ang", None, "slab", None)),
        check_vma=False,
    )
```

```python
import functools

import jax
import jax.numpy as jnp
from jax import lax
from jax.experimental import pallas as pl
from jax.experimental.pallas import tpu as pltpu
from jax.sharding import PartitionSpec as P

SMOOTHING = 0.25
MESH = pl.DeviceIdType.MESH


def kernel(
    groups,
    slabs,
    turns,
    starts_ref,
    ids_ref,
    weights_ref,
    updates_ref,
    tiles_hbm,
    volume_ref,
    next_ref,
    projection_ref,
    tiles_ref,
    wide_ref,
    scaled_ref,
    sent_ref,
    landed_ref,
    gathered_ref,
    halo_ref,
    tile_sems,
    send_sem,
    land_sems,
    spread_sem,
    gather_sems,
    halo_sems,
):
    local_angles, row_count, detector = updates_ref.shape
    tile_count, band_width, block_size = tiles_ref.shape[1:]
    share = sent_ref.shape[2]
    unit = wide_ref.shape[2]
    unit_count = wide_ref.shape[0]
    per_unit = unit // share
    unit_tiles = unit // block_size
    depth = row_count // 2
    column_blocks = detector // block_size
    halves = band_width // block_size
    me = lax.axis_index("ang")
    slab = lax.axis_index("slab")
    my_unit = me // per_unit

    def unit_at(step):
        return lax.rem(my_unit + step, unit_count)

    def tile_copy(where):
        block = pl.ds(where * unit_tiles, unit_tiles)
        return pltpu.make_async_copy(
            tiles_hbm.at[:, block], tiles_ref.at[:, block], tile_sems.at[where]
        )

    @pl.loop(1, unit_count + 1)
    def _(step):
        tile_copy(unit_at(step)).start()

    barrier = pltpu.get_barrier_semaphore()

    @pl.loop(1, groups)
    def _(step):
        peer = lax.rem(me + step, groups)
        pl.semaphore_signal(barrier, inc=1, device_id=(peer, slab), device_id_type=MESH)

    for turn in turns:
        beside = lax.rem(slab + turn, slabs)
        pl.semaphore_signal(barrier, inc=1, device_id=(me, beside), device_id_type=MESH)

    for angle in range(local_angles):
        chosen = weights_ref[ids_ref[angle]]
        scaled_ref[:, angle * detector : (angle + 1) * detector] = (
            chosen * updates_ref[angle]
        ).astype(jnp.bfloat16)

    pl.semaphore_wait(barrier, groups - 1 + len(turns))

    halo_copies = []
    for slot, turn in enumerate(turns):
        halo_copies.append(
            pltpu.make_async_remote_copy(
                src_ref=volume_ref,
                dst_ref=halo_ref.at[slot],
                send_sem=halo_sems.at[0, slot],
                recv_sem=halo_sems.at[1, slot],
                device_id=(me, lax.rem(slab + turn, slabs)),
                device_id_type=MESH,
            )
        )
        halo_copies[-1].start()

    def term_copy(owner):
        return pltpu.make_async_remote_copy(
            src_ref=sent_ref.at[owner],
            dst_ref=landed_ref.at[me],
            send_sem=send_sem.at[owner],
            recv_sem=land_sems.at[me],
            device_id=(owner, slab),
            device_id_type=MESH,
        )

    def back(where):
        tile_copy(where).wait()
        for angle in range(local_angles):
            for part in range(unit_tiles):
                index = where * unit_tiles + part
                first = starts_ref[angle, index]
                for column in range(column_blocks):
                    block = jnp.zeros((block_size, block_size), jnp.bfloat16)
                    for half in range(halves):
                        held = tiles_ref[
                            angle, index, half * block_size : (half + 1) * block_size, :
                        ]
                        block = jnp.where(first + half == column, held, block)
                    top = angle * detector + column * block_size
                    wide_ref[
                        where,
                        top : top + block_size,
                        part * block_size : (part + 1) * block_size,
                    ] = block
        term = jnp.dot(
            scaled_ref[...], wide_ref[where], preferred_element_type=jnp.float32
        ).astype(jnp.bfloat16)
        for part in range(per_unit):
            sent_ref[where * per_unit + part] = term[:, part * share : (part + 1) * share]

    @pl.loop(1, unit_count)
    def _(step):
        where = unit_at(step)
        back(where)
        for part in range(per_unit):
            term_copy(where * per_unit + part).start()

    back(my_unit)
    if per_unit > 1:
        for part in range(per_unit):
            owner = my_unit * per_unit + part

            @pl.when(owner != me)
            def _():
                term_copy(owner).start()

    landed_ref[me] = sent_ref[me]

    def land_wait(step):
        source = lax.rem(me + groups - step, groups)
        pltpu.make_async_remote_copy(
            src_ref=sent_ref.at[source],
            dst_ref=landed_ref.at[source],
            send_sem=send_sem.at[source],
            recv_sem=land_sems.at[source],
            device_id=(source, slab),
            device_id_type=MESH,
        ).wait_recv()

    pl.loop(1, groups)(land_wait)
    for halo_copy in halo_copies:
        halo_copy.wait()

    lane = lax.broadcasted_iota(jnp.int32, (share, depth), 1)
    for channel in range(2):
        rows = slice(channel * depth, (channel + 1) * depth)
        total = lax.fori_loop(
            1,
            groups,
            lambda i, acc: acc + landed_ref[i, rows, :].astype(jnp.float32),
            landed_ref[0, rows, :].astype(jnp.float32),
        )
        if share % 128:
            room = 128 - share % 128
            total = jnp.concatenate([total, jnp.zeros((depth, room), jnp.float32)], axis=1)
        total = total.T[:share]
        cells = volume_ref[:, channel, :]
        before = pltpu.roll(cells, 1, 1)
        after = pltpu.roll(cells, depth - 1, 1)
        edge_before = jnp.zeros_like(cells)
        edge_after = jnp.zeros_like(cells)
        if slabs > 1:
            lower = halo_ref[0, :, channel, :]
            upper = halo_ref[len(turns) - 1, :, channel, :]
            edge_before = jnp.where(slab > 0, pltpu.roll(lower, 1, 1), edge_before)
            edge_after = jnp.where(
                slab < slabs - 1, pltpu.roll(upper, depth - 1, 1), edge_after
            )
        before = jnp.where(lane == 0, edge_before, before)
        after = jnp.where(lane == depth - 1, edge_after, after)
        smooth = cells - SMOOTHING * (2.0 * cells - before - after)
        result = smooth + total
        if channel == 1:
            result = jnp.maximum(result, 0.0)
        next_ref[:, channel, :] = result
        if share % 128:
            room = 128 - share % 128
            result = jnp.concatenate([result, jnp.zeros((room, depth), jnp.float32)], axis=0)
        gathered_ref[me, rows, :] = result.T[:, :share].astype(jnp.bfloat16)

    inner = 4 if groups % 4 == 0 else 1
    outer = groups // inner
    my_outer, my_inner = me // inner, lax.rem(me, inner)

    def device_of(up, along):
        return lax.rem(my_outer + up, outer) * inner + lax.rem(my_inner + along, inner)

    def spread_copy(peer, slot, ticket):
        return pltpu.make_async_remote_copy(
            src_ref=gathered_ref.at[slot],
            dst_ref=gathered_ref.at[slot],
            send_sem=spread_sem.at[ticket],
            recv_sem=gather_sems.at[slot],
            device_id=(peer, slab),
            device_id_type=MESH,
        )

    for up in range(1, outer):
        spread_copy(device_of(up, 0), me, up * inner).start()
    for along in range(1, inner):
        spread_copy(device_of(0, along), me, along).start()

    def forward(where, fresh):
        for angle in range(local_angles):
            image = None
            for part in range(per_unit):
                piece = lax.dot_general(
                    gathered_ref[where * per_unit + part],
                    wide_ref[
                        where,
                        angle * detector : (angle + 1) * detector,
                        part * share : (part + 1) * share,
                    ],
                    (((1,), (1,)), ((), ())),
                    preferred_element_type=jnp.float32,
                )
                image = piece if image is None else image + piece
            if fresh:
                projection_ref[angle] = image
            else:
                projection_ref[angle] += image

    def arrived(source):
        spread_copy(source, source, 0).wait_recv()

    if per_unit == 1:
        forward(me, True)

    for up in range(1, outer):
        source = device_of(outer - up, 0)
        arrived(source)
        for along in range(1, inner):
            spread_copy(device_of(0, along), source, up * inner + along).start()
        if per_unit == 1:
            forward(source, False)

    @pl.loop(0, outer)
    def _(up):
        for along in range(1, inner):
            source = device_of(outer - up, inner - along)
            arrived(source)
            if per_unit == 1:
                forward(source, False)

    if per_unit > 1:
        forward(0, True)

        @pl.loop(1, unit_count)
        def _(where):
            forward(where, False)

    @pl.loop(1, groups)
    def _(step):
        peer = lax.rem(me + step, groups)
        term_copy(peer).wait_send()
        spread_copy(peer, me, step).wait_send()


def shards(groups, slabs, updates, interp_tiles, band_start, angle_id, angle_weight, volume):
    local_angles, channels, depth, detector = updates.shape
    tile_count, band_width, block_size = interp_tiles.shape[1:]
    share = volume.shape[0]
    row_count = channels * depth
    unit = max(share, block_size)
    unit_count = tile_count * block_size // unit
    turns = {1: (), 2: (1,)}.get(slabs, (1, slabs - 1))
    slots = max(1, len(turns))
    half = jnp.bfloat16
    vmem = pl.BlockSpec(memory_space=pltpu.VMEM)
    smem = pl.BlockSpec(memory_space=pltpu.SMEM)
    dma = pltpu.SemaphoreType.DMA
    volume_next, projection = pl.pallas_call(
        functools.partial(kernel, groups, slabs, turns),
        name="project",
        out_shape=(
            jax.ShapeDtypeStruct(volume.shape, jnp.float32),
            jax.ShapeDtypeStruct((local_angles, row_count, detector), jnp.float32),
        ),
        in_specs=[smem, smem, smem, vmem, pl.BlockSpec(memory_space=pl.ANY), vmem],
        out_specs=(vmem, vmem),
        scratch_shapes=[
            pltpu.VMEM(interp_tiles.shape, half),
            pltpu.VMEM((unit_count, local_angles * detector, unit), half),
            pltpu.VMEM((row_count, local_angles * detector), half),
            pltpu.VMEM((groups, row_count, share), half),
            pltpu.VMEM((groups, row_count, share), half),
            pltpu.VMEM((groups, row_count, share), half),
            pltpu.VMEM((slots,) + volume.shape, jnp.float32),
            dma((unit_count,)),
            dma((groups,)),
            dma((groups,)),
            dma((groups,)),
            dma((groups,)),
            dma((2, slots)),
        ],
        compiler_params=pltpu.CompilerParams(
            collective_id=0, has_side_effects=True, vmem_limit_bytes=60 * 1024 * 1024
        ),
    )(
        band_start,
        angle_id,
        angle_weight,
        updates.reshape(local_angles, row_count, detector),
        interp_tiles,
        volume,
    )
    return volume_next, projection.reshape(updates.shape)


def solution(mesh):
    placed = (
        P("ang", None, "slab", None),
        P("ang", None, None, None),
        P("ang", None),
        P("ang"),
        P(),
        P("ang", None, "slab"),
    )
    return jax.shard_map(
        functools.partial(shards, mesh.shape["ang"], mesh.shape["slab"]),
        mesh=mesh,
        in_specs=placed,
        out_specs=(P("ang", None, "slab"), P("ang", None, "slab", None)),
        check_vma=False,
    )
```
